32 devices in a mesh: groups: 2 (over x), prompt: 8 (over z, y), resp: 2 (over core).
Axes of the slice: x: 2, y: 2, z: 4, core: 2. Of those that a mesh axis runs over, the one named last changes fastest.
Arguments:
- queries: bfloat16 [16, 512, 1024], P(('groups', 'prompt'), 'resp'), parts along dimension 0, may hold values from -4096 to 4096
- grad_out: bfloat16 [16, 512, 1024], P(('groups', 'prompt'), 'resp'), parts along dimension 0, may hold values from -48 to 48
- keys_resp: bfloat16 [16, 512, 128], P(('groups', 'prompt'), 'resp'), parts along dimension 0, may hold values from -6 to 6
- values_resp: bfloat16 [16, 512, 128], P(('groups', 'prompt'), 'resp'), parts along dimension 0, may hold values from -6 to 6
- keys_prefix: bfloat16 [1024, 128], P(('groups', 'prompt')), parts along dimension 0, may hold values from -32 to 32
- values_prefix: bfloat16 [1024, 128], P(('groups', 'prompt')), parts along dimension 0, may hold values from -6 to 6
- lengths: int32 [16], P(('groups', 'prompt')), parts along dimension 0, may hold values from 1 to 512, as said below
- block_plan: int32 [16, 4], P(('groups', 'prompt'), 'resp'), parts along dimension 0, may hold values from 0 to 3, as said below
Outputs:
- query_grads: float32 [16, 512, 1024], P(('groups', 'prompt'), 'resp'), parts along dimension 0
- prefix_keygrad: float32 [1024, 128], P(('groups', 'prompt', 'resp')), parts along dimension 0
- prefix_valgrad: float32 [1024, 128], P(('groups', 'prompt', 'resp')), parts along dimension 0
- reply_keygrad: float32 [16, 512, 128], P(('groups', 'prompt'), 'resp'), parts along dimension 0
- reply_valgrad: float32 [16, 512, 128], P(('groups', 'prompt'), 'resp'), parts along dimension 0
The draws below stay inside these ranges and needn't reach their ends.
There are 2 independent parts, one for each index of `groups`. The reference program is written for one: setup_inputs(seed, part) draws one part's arguments, and reference() takes and returns one part's arrays. A program takes and returns all parts, laid end to end along the dimension named above; each array names one. Nothing has to cross between parts.
Inputs may be any that keep to these rules, and one draw needn't show every extreme that they name: `lengths`: one response has exactly 512 live positions. `block_plan`: each row is a permutation of 0 to 3; for every m, blocks 2 * m and 2 * m + 1 stand in different halves of the row.
All inputs are finite; a program needn't handle non-finite values.
Results may differ from the reference program's by a relative error of at most 0.0029.
Values may be sent and summed in bfloat16 or wider, within the bound.
No kernel may reach another device: no remote copies, remote signals or barrier semaphores. Data moves between devices by JAX's collectives and lax.ppermute only.
A program may use at most 64 MiB of HBM per device.

```python
import jax
import jax.numpy as jnp
from jax import lax

HEAD = 128
HEADS = 8
RBLK = 128
P_SIZE = 512
NRESP = 8
LMAX = 512
NBLK = 4


def prefix_draw(key):
    normal_draw = jnp.clip(jax.random.normal(jax.random.fold_in(key, 101), (P_SIZE, HEAD), jnp.float32), -5.0, 5.0)
    return normal_draw


def draw_keys_prefix(key, part):
    return prefix_draw(key).astype(jnp.bfloat16)


def draw_queries(key, part):
    normal_draw = jnp.clip(jax.random.normal(jax.random.fold_in(key, 201), (NRESP, LMAX, HEADS, HEAD), jnp.float32), -5.0, 5.0)
    return normal_draw.reshape(NRESP, LMAX, HEADS * HEAD).astype(jnp.bfloat16)


def draw_lengths(key, part):
    lengths_draw = jax.random.randint(jax.random.fold_in(key, 401), (NRESP,), 1, LMAX + 1, jnp.int32)
    longest = jax.random.randint(jax.random.fold_in(key, 402), (), 0, NRESP, jnp.int32)
    return jnp.where(jnp.arange(NRESP, dtype=jnp.int32) == longest, LMAX, lengths_draw).astype(jnp.int32)


def draw_block_plan(key, part):
    half_count = NBLK // 2
    coin_flip = jax.random.randint(jax.random.fold_in(key, 301), (NRESP, half_count), 0, 2, jnp.int32)
    pair_start = 2 * jnp.arange(half_count, dtype=jnp.int32)
    to_first = pair_start[None, :] + coin_flip
    to_second = pair_start[None, :] + 1 - coin_flip
    halves = jnp.stack([to_first, to_second], 1)
    subkeys = jax.random.split(jax.random.fold_in(key, 302), NRESP * 2)
    orders = jax.vmap(lambda subkey: jax.random.permutation(subkey, half_count))(subkeys).reshape(NRESP, 2, half_count)
    placed = jnp.take_along_axis(halves, orders.astype(jnp.int32), axis=2)
    return placed.reshape(NRESP, NBLK).astype(jnp.int32)


def shard_levels(key, dims, cuts, least, top_value):
    loudness = 1.0
    for dim, parts in cuts:
        draws = jax.random.uniform(jax.random.fold_in(jax.random.fold_in(key, 6), dim), (parts,), jnp.float32, least / len(cuts), top_value / len(cuts))
        loudness = loudness * jnp.repeat(jnp.exp(draws), dims[dim] // parts).reshape((-1,) + (1,) * (len(dims) - 1 - dim))
    return loudness


def noise(rng, extent, deviation, most, cuts=(), held_as=jnp.bfloat16):
    values = jax.random.normal(rng, extent, jnp.float32) * deviation
    if len(cuts) > 0:
        values = shard_levels(rng, extent, cuts, -0.22, 0.18) * values
    return jnp.clip(values, min=-most, max=most).astype(held_as)


def setup_inputs(seed: int = 0, part: int = 0) -> dict:
    arg_keys = jax.random.split(jax.random.key(seed), 9)
    part_keys = jax.random.split(jax.random.fold_in(arg_keys[8], part), 9)
    return {
        "queries": draw_queries(jax.random.fold_in(jax.random.fold_in(arg_keys[8], part), 71), part),
        "grad_out": noise(part_keys[1], (NRESP, LMAX, HEADS * HEAD), 8.0, 48.0, ((0, 8), (1, 2))),
        "keys_resp": noise(part_keys[2], (NRESP, LMAX, HEAD), 1.0, 6.0, ((0, 8), (1, 2))),
        "values_resp": noise(part_keys[3], (NRESP, LMAX, HEAD), 1.0, 6.0, ((0, 8), (1, 2))),
        "keys_prefix": draw_keys_prefix(jax.random.fold_in(jax.random.fold_in(arg_keys[8], part), 71), part),
        "values_prefix": noise(part_keys[5], (P_SIZE, HEAD), 1.0, 6.0, ((0, 8),)),
        "lengths": draw_lengths(jax.random.fold_in(jax.random.fold_in(arg_keys[8], part), 71), part),
        "block_plan": draw_block_plan(jax.random.fold_in(jax.random.fold_in(arg_keys[8], part), 71), part),
    }


def reference(queries, grad_out, keys_resp, values_resp, keys_prefix, values_prefix, lengths, block_plan):
    score_scale = HEAD ** -0.5
    prefix_keys = keys_prefix.astype(jnp.float32)
    prefix_values = values_prefix.astype(jnp.float32)
    key_index = jnp.arange(P_SIZE + LMAX, dtype=jnp.int32)
    relative = key_index - P_SIZE
    positions = jnp.arange(LMAX, dtype=jnp.int32)

    def per_response(totals, block_item):
        query_rows, grad_rows, reply_keys, reply_values, length = block_item
        all_keys = jnp.concatenate([prefix_keys, reply_keys.astype(jnp.float32)], 0)
        all_values = jnp.concatenate([prefix_values, reply_values.astype(jnp.float32)], 0)
        query_heads = query_rows.astype(jnp.float32).reshape(LMAX, HEADS, HEAD)
        live_rows = positions < length
        grad_heads = jnp.where(live_rows[:, None, None], grad_rows.astype(jnp.float32).reshape(LMAX, HEADS, HEAD), jnp.float32(0.0))
        visible = (key_index[None, :] < P_SIZE) | ((relative[None, :] <= positions[:, None]) & (relative[None, :] < length))
        scores = jnp.einsum('rhd,kd->rhk', query_heads, all_keys) * score_scale
        scores = jnp.where(visible[:, None, :], scores, -jnp.inf)
        row_max = jnp.max(scores, -1, keepdims=True)
        exponent = jnp.exp(scores - row_max)
        weights = exponent / jnp.sum(exponent, -1, keepdims=True)
        grad_weight = jnp.einsum('rhd,kd->rhk', grad_heads, all_values)
        row_inner = jnp.sum(weights * grad_weight, -1, keepdims=True)
        grad_score = lax.optimization_barrier((weights * (grad_weight - row_inner)).astype(jnp.bfloat16)).astype(jnp.float32)
        rounded_weights = lax.optimization_barrier(weights.astype(jnp.bfloat16)).astype(jnp.float32)
        grad_q = jnp.einsum('rhk,kd->rhd', grad_score, all_keys) * score_scale
        grad_k = jnp.einsum('rhk,rhd->kd', grad_score, query_heads) * score_scale
        grad_v = jnp.einsum('rhk,rhd->kd', rounded_weights, grad_heads)
        new_totals = (totals[0] + grad_k[:P_SIZE], totals[1] + grad_v[:P_SIZE])
        return new_totals, (grad_q.reshape(LMAX, HEADS * HEAD), grad_k[P_SIZE:], grad_v[P_SIZE:])

    zeros = jnp.zeros((P_SIZE, HEAD), jnp.float32)
    totals, outputs = lax.scan(per_response, (zeros, zeros), (queries, grad_out, keys_resp, values_resp, lengths))
    natural_grads, reply_keygrad, reply_valgrad = outputs
    blocks = natural_grads.reshape(NRESP, NBLK, RBLK, HEADS * HEAD)
    chosen = jnp.take_along_axis(blocks, block_plan.astype(jnp.int32)[:, :, None, None], axis=1)
    query_grads = chosen.reshape(NRESP, LMAX, HEADS * HEAD)
    return query_grads, totals[0], totals[1], reply_keygrad, reply_valgrad
```

```python
import jax
import jax.numpy as jnp
from jax import lax
from jax.experimental import pallas as pl
from jax.experimental.pallas import tpu as pltpu
from jax.sharding import PartitionSpec as P


RBLK = 128
PAIR = 2
ROWS = PAIR * RBLK
LOG2E = 1.4426950408889634
COVER = 10**10
F32 = jnp.float32
BF16 = jnp.bfloat16


def nt(a, b):
    return lax.dot_general(a, b, (((1,), (1,)), ((), ())), preferred_element_type=F32)


def nn(a, b):
    return lax.dot_general(a, b, (((1,), (0,)), ((), ())), preferred_element_type=F32)


def tn(a, b):
    return lax.dot_general(a, b, (((0,), (0,)), ((), ())), preferred_element_type=F32)


def fold(x, op):
    return op(x.reshape(x.shape[0] // 8, 8, x.shape[1]), axis=0)


def pieces(count):
    out = []
    at = 0
    while at < count:
        step = min(2 * RBLK, count - at)
        out.append((at, step))
        at += step
    return out


def call(body, ins, outs, scratch, limit, cost=None, far=False):
    vmem = pl.BlockSpec(memory_space=pltpu.VMEM)
    return pl.pallas_call(
        body,
        in_specs=[vmem] * len(ins),
        out_specs=[pl.BlockSpec(memory_space=pl.ANY) if far else vmem] * len(outs),
        out_shape=[jax.ShapeDtypeStruct(*o) for o in outs],
        scratch_shapes=scratch,
        compiler_params=pltpu.CompilerParams(vmem_limit_bytes=limit),
        cost_estimate=cost,
    )(*ins)


OWN, LEN, CORE, SLOT = 0, 2, 3, 4


def scalars(plan_ref, len_ref, blocks):
    core = lax.axis_index("resp")
    plan = plan_ref[...]
    length = len_ref[...]
    first_own = plan[0, 0] // blocks == core
    return (
        jnp.where(first_own, plan[0, 0], plan[0, 1]),
        jnp.where(first_own, plan[0, 1], plan[0, 0]),
        length[0, 0],
        core,
        jnp.where(first_own, 0, 1),
    )


def spread_scalars(info, out):
    for at, x in enumerate(info):
        out[at : at + 1, :] = jnp.full((1, out.shape[1]), x, jnp.int32)


def read_scalars(ref):
    x = ref[...]
    return [x[at, 0] for at in range(SLOT + 1)]


class Shape:
    def __init__(self, q, k, core_count):
        self.slots, self.width = q.shape
        self.head = k.shape[1]
        self.heads = self.width // self.head
        self.blocks = self.slots // RBLK
        self.total = self.slots * core_count
        self.kinds = self.total // RBLK
        self.lanes = self.heads * RBLK
        self.pairs = self.heads // PAIR
        self.scale = self.head ** (-0.5)
        self.factor = self.scale * LOG2E
        self.limit = 12 << 20


def when_live(info, item, fn, dead=None):
    b = info[OWN + item]
    live = b * RBLK < info[LEN]

    @pl.when(live)
    def _():
        fn(b)

    if dead is not None:

        @pl.when(jnp.logical_not(live))
        def _():
            dead()


def for_kind(z, b, fn):
    for kind in range(z.kinds):

        @pl.when(b == kind)
        def _():
            fn(kind)


def score(z, keys, values, parts, q2, g2, cols, e_ref, p_ref, st_ref, seen=None):
    def scores(at, step):
        s = nt(keys(at, step), q2)
        if seen is not None and (at, step) == parts[-1]:
            cut = step - RBLK
            diag = jnp.where(seen, s[cut:], -jnp.inf)
            s = jnp.concatenate([s[:cut], diag], 0) if cut else diag
        return s

    top = jnp.full((8, ROWS), -jnp.inf, F32)
    for at, step in parts:
        top = jnp.maximum(top, fold(scores(at, step), jnp.max))
    m = jnp.max(top, axis=0, keepdims=True)
    l8 = jnp.zeros((8, ROWS), F32)
    i8 = jnp.zeros((8, ROWS), F32)
    for at, step in parts:
        dp = nt(values(at, step), g2)
        e = jnp.exp2((scores(at, step) - m) * z.factor)
        e_ref[pl.ds(at, step), cols] = e
        p_ref[pl.ds(at, step), cols] = dp
        l8 = l8 + fold(e, jnp.sum)
        i8 = i8 + fold(e * dp, jnp.sum)
    st_ref[0:1, cols] = m
    st_ref[1:2, cols] = jnp.sum(l8, axis=0, keepdims=True)
    st_ref[2:3, cols] = jnp.sum(i8, axis=0, keepdims=True)


def mask_dead(z, info, b, g_ref):
    t = b * RBLK + lax.broadcasted_iota(jnp.int32, (RBLK, z.head), 0)

    @pl.when((b + 1) * RBLK > info[LEN])
    def _():
        for h in range(z.heads):
            rows = pl.ds(h * RBLK, RBLK)
            part = g_ref[rows, :]
            g_ref[rows, :] = jnp.where(t < info[LEN], part, jnp.zeros_like(part))


def make_kernel(core_count, slots, width, head, prefix_len):
    heads = width // head
    total = slots * core_count
    blocks = slots // RBLK
    all_blocks = blocks * core_count
    keys = prefix_len + total
    pair = PAIR
    scale = head ** (-0.5)

    def kernel(plan, length_ref, core_ref, qo, qx, go, gx, kp, vp, ko, kx, vo, vx,
               dq_out, pre_out, keep_out, send_out,
               k_all, v_all, acc_k, acc_v, q_blk, g_blk, s_buf, p_buf):
        core = core_ref[0]
        other = 1 - core
        length = length_ref[0]
        k_all[pl.ds(0, prefix_len), :] = kp[...]
        v_all[pl.ds(0, prefix_len), :] = vp[...]
        mine = pl.multiple_of(prefix_len + core * slots, RBLK)
        theirs = pl.multiple_of(prefix_len + other * slots, RBLK)
        k_all[pl.ds(mine, slots), :] = ko[...]
        k_all[pl.ds(theirs, slots), :] = kx[...]
        v_all[pl.ds(mine, slots), :] = vo[...]
        v_all[pl.ds(theirs, slots), :] = vx[...]
        acc_k[...] = jnp.zeros_like(acc_k)
        acc_v[...] = jnp.zeros_like(acc_v)

        def load(src_q, src_g, local_row, first):
            for h in range(heads):
                q_blk[pl.ds(h * RBLK, RBLK), :] = src_q[pl.ds(local_row, RBLK), pl.ds(h * head, head)]
                g = src_g[pl.ds(local_row, RBLK), pl.ds(h * head, head)]
                t = first + lax.broadcasted_iota(jnp.int32, (RBLK, head), 0)
                g_blk[pl.ds(h * RBLK, RBLK), :] = jnp.where(t < length, g, jnp.zeros_like(g))

        def one_block(slot, b_static, first):
            key_count = prefix_len + (b_static + 1) * RBLK
            rows = pair * RBLK
            sizes = []
            at = 0
            while at < key_count:
                step = min(2 * RBLK, key_count - at)
                sizes.append((at, step))
                at += step
            u = lax.broadcasted_iota(jnp.int32, (RBLK, rows), 0)
            t = lax.broadcasted_iota(jnp.int32, (RBLK, rows), 1) % RBLK
            seen = u <= jnp.minimum(t, length - 1 - first)

            def head_pair(hp, carry):
                at_row = pl.multiple_of(hp * rows, rows)
                q2 = q_blk[pl.ds(at_row, rows), :]
                g2 = g_blk[pl.ds(at_row, rows), :]
                top = jnp.full((8, rows), -jnp.inf, jnp.float32)
                for at, step in sizes:
                    s = nt(k_all[pl.ds(at, step), :], q2)
                    if at + step == key_count:
                        cut = step - RBLK
                        diag = jnp.where(seen, s[cut:], -jnp.inf)
                        s = jnp.concatenate([s[:cut], diag], 0) if cut else diag
                    s_buf[pl.ds(at, step), :] = s
                    top = jnp.maximum(top, fold(s, jnp.max))
                m = jnp.max(top, axis=0, keepdims=True)
                l8 = jnp.zeros((8, rows), jnp.float32)
                i8 = jnp.zeros((8, rows), jnp.float32)
                for at, step in sizes:
                    dp = nt(v_all[pl.ds(at, step), :], g2)
                    e = jnp.exp2((s_buf[pl.ds(at, step), :] - m) * (scale * LOG2E))
                    s_buf[pl.ds(at, step), :] = e
                    p_buf[pl.ds(at, step), :] = dp
                    l8 = l8 + fold(e, jnp.sum)
                    i8 = i8 + fold(e * dp, jnp.sum)
                rl = 1.0 / jnp.sum(l8, axis=0, keepdims=True)
                inner = jnp.sum(i8, axis=0, keepdims=True) * rl
                dq = jnp.zeros((rows, head), jnp.float32)
                for at, step in sizes:
                    w = s_buf[pl.ds(at, step), :] * rl
                    ds = (w * (p_buf[pl.ds(at, step), :] - inner)).astype(jnp.bfloat16)
                    acc_v[pl.ds(at, step), :] += nn(w.astype(jnp.bfloat16), g2)
                    acc_k[pl.ds(at, step), :] += nn(ds, q2)
                    dq = dq + tn(ds, k_all[pl.ds(at, step), :])
                dq = dq * scale
                for j in range(pair):
                    lane = pl.multiple_of((hp * pair + j) * head, head)
                    dq_out[pl.ds(slot * RBLK, RBLK), pl.ds(lane, head)] = dq[j * RBLK : (j + 1) * RBLK]
                return carry

            lax.fori_loop(0, heads // pair, head_pair, 0)

        for slot in range(blocks):
            b = plan[slot]
            first = b * RBLK
            local_row = pl.multiple_of((b % blocks) * RBLK, RBLK)
            live = first < length

            @pl.when(live & (b // blocks == core))
            def _():
                load(qo, go, local_row, first)

            @pl.when(live & (b // blocks != core))
            def _():
                load(qx, gx, local_row, first)

            for kind in range(all_blocks):

                @pl.when(live & (b == kind))
                def _():
                    one_block(slot, kind, first)

            @pl.when(jnp.logical_not(live))
            def _():
                dq_out[pl.ds(slot * RBLK, RBLK), :] = jnp.zeros((RBLK, width), jnp.float32)

        pre_out[:, pl.ds(0, head)] = (acc_k[pl.ds(0, prefix_len), :] * scale).astype(jnp.bfloat16)
        pre_out[:, pl.ds(head, head)] = acc_v[pl.ds(0, prefix_len), :].astype(jnp.bfloat16)
        keep_out[:, pl.ds(0, head)] = acc_k[pl.ds(mine, slots), :] * scale
        keep_out[:, pl.ds(head, head)] = acc_v[pl.ds(mine, slots), :]
        send_out[:, pl.ds(0, head)] = acc_k[pl.ds(theirs, slots), :] * scale
        send_out[:, pl.ds(head, head)] = acc_v[pl.ds(theirs, slots), :]

    smem = pl.BlockSpec(memory_space=pltpu.SMEM)
    vmem = pl.BlockSpec(memory_space=pltpu.VMEM)
    f32, bf16 = jnp.float32, jnp.bfloat16
    return pl.pallas_call(
        kernel,
        in_specs=[smem] * 3 + [vmem] * 10,
        out_specs=[vmem] * 4,
        out_shape=[
            jax.ShapeDtypeStruct((slots, width), f32),
            jax.ShapeDtypeStruct((prefix_len, 2 * head), bf16),
            jax.ShapeDtypeStruct((slots, 2 * head), f32),
            jax.ShapeDtypeStruct((slots, 2 * head), f32),
        ],
        scratch_shapes=[
            pltpu.VMEM((keys, head), bf16),
            pltpu.VMEM((keys, head), bf16),
            pltpu.VMEM((keys, head), f32),
            pltpu.VMEM((keys, head), f32),
            pltpu.VMEM((heads * RBLK, head), bf16),
            pltpu.VMEM((heads * RBLK, head), bf16),
            pltpu.VMEM((keys, pair * RBLK), f32),
            pltpu.VMEM((keys, pair * RBLK), f32),
        ],
        name="attention_backward",
    )


def pack(z, kp, vp):
    chunk = kp.shape[0]
    wide = [lax.pad(x, jnp.zeros((), x.dtype), ((0, 0, 0), side)) for x, side in ((kp, (0, z.head, 0)), (vp, (z.head, 0, 0)))]
    lane = lax.broadcasted_iota(jnp.int32, (chunk, 2 * z.head), 1)
    both = jnp.where(lane < z.head, *wide)

    def body(x, out):
        out[...] = x[...]

    cost = pl.CostEstimate(flops=COVER, transcendentals=0, bytes_accessed=4 * chunk * z.head)
    return call(body, (both,), [((chunk, 2 * z.head), BF16)], [], z.limit, cost)[0]


def reply_item(z, info_ref, item, src_q, src_g, k_all, v_all, qw, gw, out):
    u = lax.broadcasted_iota(jnp.int32, (RBLK, ROWS), 0)
    t = lax.broadcasted_iota(jnp.int32, (RBLK, ROWS), 1) % RBLK

    def kinds(kind):
        seen = u <= jnp.minimum(t, info_ref[LEN] - 1 - kind * RBLK)
        for hp in range(z.pairs):
            cols = pl.ds(hp * ROWS, ROWS)
            score(z, lambda at, step: k_all[pl.ds(at, step), :], lambda at, step: v_all[pl.ds(at, step), :],
                  pieces((kind + 1) * RBLK), qw[cols, :], gw[cols, :], cols, *out, seen)

    def go(b):
        row = pl.multiple_of((b % z.blocks) * RBLK, RBLK)
        for h in range(z.heads):
            qw[pl.ds(h * RBLK, RBLK), :] = src_q[pl.ds(row, RBLK), pl.ds(h * z.head, z.head)]
            gw[pl.ds(h * RBLK, RBLK), :] = src_g[pl.ds(row, RBLK), pl.ds(h * z.head, z.head)]
        mask_dead(z, info_ref, b, gw)
        for_kind(z, b, kinds)

    when_live(info_ref, item, go)


def reply_shapes(z):
    return [((z.lanes, z.head), BF16)] * 2 + [((z.total, z.lanes), F32), ((z.total, z.lanes), F32), ((8, z.lanes), F32)]


def reply_own(z, plan, length, q, g, k, kx, v, vx):
    def body(plan_ref, len_ref, qo, go, ko, kx_, vo, vx_, info_out, k_all, v_all, q0, g0, *res):
        info_ref = scalars(plan_ref, len_ref, z.blocks)
        spread_scalars(info_ref, info_out)
        core = info_ref[CORE]
        mine = pl.multiple_of(core * z.slots, RBLK)
        theirs = pl.multiple_of((1 - core) * z.slots, RBLK)
        k_all[pl.ds(mine, z.slots), :] = ko[...]
        k_all[pl.ds(theirs, z.slots), :] = kx_[...]
        v_all[pl.ds(mine, z.slots), :] = vo[...]
        v_all[pl.ds(theirs, z.slots), :] = vx_[...]
        reply_item(z, info_ref, 0, qo, go, k_all, v_all, q0, g0, res)

    out = call(body, (plan, length, q, g, k, kx, v, vx),
               [((8, z.head), jnp.int32)] + [((z.total, z.head), BF16)] * 2 + reply_shapes(z), [], z.limit)
    return out[0], out[1], out[2], out[3], out[4], out[5:8]


def reply_other(z, info, qx, gx, k_all, v_all):
    def body(info_in, qx_, gx_, k_all_, v_all_, q1, g1, *res):
        reply_item(z, read_scalars(info_in), 1, qx_, gx_, k_all_, v_all_, q1, g1, res)

    out = call(body, (info, qx, gx, k_all, v_all), reply_shapes(z), [], z.limit)
    return out[0], out[1], out[2:5]


def front_scores(z, info, kv, qs, gs):
    half = kv.shape[0]

    def body(info_in, kv_, q0, q1, g0, g1, *res):
        info_ref = read_scalars(info_in)
        for item, (qw, gw) in enumerate(((q0, g0), (q1, g1))):
            out = res[3 * item : 3 * item + 3]

            def go(b):
                for hp in range(z.pairs):
                    cols = pl.ds(hp * ROWS, ROWS)
                    score(z, lambda at, step: kv_[pl.ds(at, step), pl.ds(0, z.head)],
                          lambda at, step: kv_[pl.ds(at, step), pl.ds(z.head, z.head)],
                          pieces(half), qw[cols, :], gw[cols, :], cols, *out)

            when_live(info_ref, item, go)

    one = [((half, z.lanes), F32), ((half, z.lanes), F32), ((8, z.lanes), F32)]
    out = call(body, (info, kv, *qs, *gs), one + one, [], z.limit)
    return out[0:3], out[3:6]


def rounded(er, pr, lift, inner, cols, w_ref, ds_ref):
    for at, step in pieces(er.shape[0]):
        rows = pl.ds(at, step)
        w = er[rows, cols] * lift
        w_ref[rows, cols] = w.astype(BF16)
        ds_ref[rows, cols] = (w * (pr[rows, cols] - inner)).astype(BF16)


def add_sums(z, out, w_ref, ds_ref, qw, gw):
    out[:, pl.ds(0, z.head)] += nn(ds_ref[...], qw[...]) * z.scale
    out[:, pl.ds(z.head, z.head)] += nn(w_ref[...], gw[...])


def prompt_send(z, info, kv, qs, gs, front, reply):
    half = kv.shape[0]

    def body(info_in, kv_, q0, q1, g0, g1, sa0, sa1, sr0, sr1, send, ds0, ds1, fac0, fac1, w_ref, e_ref, p_ref, st_ref):
        info_ref = read_scalars(info_in)
        send[...] = jnp.zeros_like(send)
        for item, (qw, gw, sa, sr, ds_ref, fac) in enumerate(((q0, g0, sa0, sr0, ds0, fac0), (q1, g1, sa1, sr1, ds1, fac1))):

            def go(b):
                for hp in range(z.pairs):
                    cols = pl.ds(hp * ROWS, ROWS)
                    score(z, lambda at, step: kv_[pl.ds(at, step), pl.ds(0, z.head)],
                          lambda at, step: kv_[pl.ds(at, step), pl.ds(z.head, z.head)],
                          pieces(half), qw[cols, :], gw[cols, :], cols, e_ref, p_ref, st_ref)
                    sets = (sr[0:3, cols], sa[0:3, cols], st_ref[0:3, cols])
                    m = jnp.maximum(jnp.maximum(sets[0][0:1], sets[1][0:1]), sets[2][0:1])
                    lifts = [jnp.exp2((x[0:1] - m) * z.factor) for x in sets]
                    rl = 1.0 / sum(x[1:2] * f for x, f in zip(sets, lifts))
                    inner = sum(x[2:3] * f for x, f in zip(sets, lifts)) * rl
                    for at, lift in enumerate(lifts):
                        fac[at : at + 1, cols] = lift * rl
                    fac[3:4, cols] = inner
                    rounded(e_ref, p_ref, lifts[2] * rl, inner, cols, w_ref, ds_ref)
                add_sums(z, send, w_ref, ds_ref, qw, gw)

            when_live(info_ref, item, go)

    out = call(
        body, (info, kv, *qs, *gs, front[0][2], front[1][2], reply[0][2], reply[1][2]),
        [((half, 2 * z.head), F32)] + [((half, z.lanes), BF16)] * 2 + [((8, z.lanes), F32)] * 2,
        [pltpu.VMEM((half, z.lanes), BF16), pltpu.VMEM((half, z.lanes), F32), pltpu.VMEM((half, z.lanes), F32),
         pltpu.VMEM((8, z.lanes), F32)],
        z.limit,
    )
    return out[0], out[1:3], out[3:5]


def prompt_keep(z, info, qs, gs, front, fac):
    half = front[0][0].shape[0]

    def body(info_in, q0, q1, g0, g1, e0, p0, e1, p1, f0, f1, keep, ds0, ds1, w_ref):
        info_ref = read_scalars(info_in)
        keep[...] = jnp.zeros_like(keep)
        for item, (qw, gw, er, pr, fac_, ds_ref) in enumerate(((q0, g0, e0, p0, f0, ds0), (q1, g1, e1, p1, f1, ds1))):

            def go(b):
                for hp in range(z.pairs):
                    cols = pl.ds(hp * ROWS, ROWS)
                    rounded(er, pr, fac_[1:2, cols], fac_[3:4, cols], cols, w_ref, ds_ref)
                add_sums(z, keep, w_ref, ds_ref, qw, gw)

            when_live(info_ref, item, go)

    out = call(
        body, (info, *qs, *gs, *front[0][:2], *front[1][:2], *fac),
        [((half, 2 * z.head), F32)] + [((half, z.lanes), BF16)] * 2,
        [pltpu.VMEM((half, z.lanes), BF16)],
        z.limit,
    )
    return out[0], out[1:3]


def split_rows(z, parts):
    rows, width = parts[0].shape
    half = rows // z.core_count

    def body(*refs):
        core = lax.axis_index("resp")
        keep, send = refs[-2:]
        for out, at in ((keep, core), (send, 1 - core)):
            here = pl.ds(pl.multiple_of(at * half, half), half)
            out[...] = sum(x[here, :].astype(F32) for x in refs[:-2])

    return call(body, parts, [((half, width), F32)] * 2, [], z.limit)


def rest_reply(z, info, qs, gs, reply, fac):
    def body(info_in, q0, q1, g0, g1, e0, p0, e1, p1, f0, f1, keep, send, d0, d1, acc_k, acc_v, w_ref):
        info_ref = read_scalars(info_in)
        acc_k[...] = jnp.zeros_like(acc_k)
        acc_v[...] = jnp.zeros_like(acc_v)
        for item, (qw, gw, er, pr, fac_, d_ref) in enumerate(((q0, g0, e0, p0, f0, d0), (q1, g1, e1, p1, f1, d1))):

            def kinds(kind):
                count = (kind + 1) * RBLK
                for hp in range(z.pairs):
                    cols = pl.ds(hp * ROWS, ROWS)
                    lift = fac_[0:1, cols]
                    inner = fac_[3:4, cols]
                    for at, step in pieces(count):
                        w = er[pl.ds(at, step), cols] * lift
                        w_ref[pl.ds(at, step), cols] = w.astype(BF16)
                        d_ref[pl.ds(at, step), cols] = (w * (pr[pl.ds(at, step), cols] - inner)).astype(BF16)
                acc_v[pl.ds(0, count), :] += nn(w_ref[pl.ds(0, count), :], gw[...])
                acc_k[pl.ds(0, count), :] += nn(d_ref[pl.ds(0, count), :], qw[...])

            when_live(info_ref, item, lambda b: for_kind(z, b, kinds))
        core = info_ref[CORE]
        mine = pl.multiple_of(core * z.slots, RBLK)
        theirs = pl.multiple_of((1 - core) * z.slots, RBLK)
        keep[:, pl.ds(0, z.head)] = acc_k[pl.ds(mine, z.slots), :] * z.scale
        keep[:, pl.ds(z.head, z.head)] = acc_v[pl.ds(mine, z.slots), :]
        send[:, pl.ds(0, z.head)] = acc_k[pl.ds(theirs, z.slots), :] * z.scale
        send[:, pl.ds(z.head, z.head)] = acc_v[pl.ds(theirs, z.slots), :]

    out = call(
        body, (info, *qs, *gs, *reply[0][:2], *reply[1][:2], *fac),
        [((z.slots, 2 * z.head), F32)] * 2 + [((z.total, z.lanes), BF16)] * 2,
        [pltpu.VMEM((z.total, z.head), F32)] * 2 + [pltpu.VMEM((z.total, z.lanes), BF16)],
        z.limit,
    )
    return out[0], out[1], out[2:4]


def query_block(z, kind, kva, kvb, kr, kept, sent, d, out, done=None):
    count = (kind + 1) * RBLK
    head = pl.ds(0, z.head)
    sides = [(kr[pl.ds(0, count), :].T, d, count), (kva[:, head].T, kept, kva.shape[0]), (kvb[:, head].T, sent, kvb.shape[0])]
    for hp in range(z.pairs):
        cols = pl.ds(hp * ROWS, ROWS)
        dq = sum(nn(keys, ds[pl.ds(0, rows), cols]) for keys, ds, rows in sides)
        dq = (dq * z.scale).T
        for j in range(PAIR):
            out[:, pl.ds((hp * PAIR + j) * z.head, z.head)] = dq[j * RBLK : (j + 1) * RBLK]
        if done is not None:
            done(hp)


def query_own(z, info, kva, kvb, k_all, kept, sent, dr):
    def body(info_in, kva_, kvb_, kr, kept_, sent_, d_, out):
        def dead():
            out[...] = jnp.zeros_like(out)

        when_live(read_scalars(info_in), 0,
                  lambda b: for_kind(z, b, lambda kind: query_block(z, kind, kva_, kvb_, kr, kept_, sent_, d_, out)), dead)

    return call(body, (info, kva, kvb, k_all, kept, sent, dr), [((RBLK, z.width), F32)], [], z.limit)[0]


def query_other(z, info, kva, kvb, k_all, kept, sent, dr, first):
    wide = z.width // z.pairs

    def body(info_in, kva_, kvb_, kr, kept_, sent_, d_, first_, dq_hbm, out, sems):
        info_ref = read_scalars(info_in)
        slot = info_ref[SLOT]

        def copy(src, at_slot, hp, sem):
            cols = pl.ds(hp * wide, wide)
            return pltpu.make_async_copy(
                src.at[:, cols], dq_hbm.at[pl.ds(pl.multiple_of(at_slot * RBLK, RBLK), RBLK), cols], sems.at[sem, hp])

        for hp in range(z.pairs):
            copy(first_, slot, hp, 0).start()

        def send(hp):
            copy(out, 1 - slot, hp, 1).start()

        def dead():
            out[...] = jnp.zeros_like(out)
            for hp in range(z.pairs):
                send(hp)

        when_live(info_ref, 1,
                  lambda b: for_kind(z, b, lambda kind: query_block(z, kind, kva_, kvb_, kr, kept_, sent_, d_, out, send)), dead)
        for hp in range(z.pairs):
            copy(first_, slot, hp, 0).wait()
            copy(out, 1 - slot, hp, 1).wait()

    return call(body, (info, kva, kvb, k_all, kept, sent, dr, first), [((z.slots, z.width), F32)],
                [pltpu.VMEM((RBLK, z.width), F32), pltpu.SemaphoreType.DMA((2, z.pairs))], z.limit, far=True)[0]


def finish(z, here, last, keep, back):
    def body(here_, last_, keep_, back_, pk, pv, rk, rv):
        for at, (a, b) in enumerate(((pk, rk), (pv, rv))):
            cols = pl.ds(at * z.head, z.head)
            a[...] = here_[:, cols] + last_[:, cols]
            b[...] = keep_[:, cols] + back_[:, cols]

    outs = [((x.shape[0], z.head), F32) for x in (here, here, keep, keep)]
    out = call(body, (here, last, keep, back), outs, [], z.limit)
    return out[0:2], out[2:4]


def staged(z, q, g, k, v, kp, vp, lengths, plan, ring, swap):
    cores = z.core_count
    rounds = ring // cores
    far = [[ring - cores + c - cores * at for at in range(rounds)] for c in range(cores)]
    far[-1][:2] = far[-1][1::-1]

    def pairs(at):
        return [(i * cores + c, (i ^ far[c][at]) * cores + c) for i in range(ring) for c in range(cores)]

    chunk = kp.shape[0]
    axes = ("prompt", "resp")
    have = pack(z, kp, vp)
    mine = jnp.concatenate([lax.ppermute(have, axes, pairs(at)) for at in range(rounds)], 0)
    theirs = lax.ppermute(mine, "resp", swap)
    kx, vx, qx, gx = (lax.ppermute(x, "resp", swap) for x in (k, v, q, g))
    info, k_all, v_all, q0, g0, own = reply_own(z, plan, lengths.reshape(1, 1), q, g, k, kx, v, vx)
    q1, g1, received = reply_other(z, info, qx, gx, k_all, v_all)
    qs, gs, reply = (q0, q1), (g0, g1), (own, received)
    front = front_scores(z, info, mine, qs, gs)
    send, sent, fac = prompt_send(z, info, theirs, qs, gs, front, reply)
    other = lax.ppermute(send, "resp", swap)
    kept_sum, kept = prompt_keep(z, info, qs, gs, front, fac)
    total = (kept_sum + other).astype(BF16)
    parts = [lax.ppermute(total[at * chunk : (at + 1) * chunk], axes, pairs(at)) for at in range(rounds)]
    here, there = split_rows(z, parts)
    last = lax.ppermute(there, "resp", swap)
    keep, away, drs = rest_reply(z, info, qs, gs, reply, fac)
    back = lax.ppermute(away, "resp", swap)
    dq = query_own(z, info, mine, theirs, k_all, kept[0], sent[0], drs[0])
    dq = query_other(z, info, mine, theirs, k_all, kept[1], sent[1], drs[1], dq)
    return dq, *finish(z, here, last, keep, back)


def local(queries, grad_out, keys_resp, values_resp, keys_prefix, values_prefix, lengths, block_plan):
    core_count = lax.axis_size("resp")
    ring = lax.axis_size("prompt")
    chunk, head = keys_prefix.shape
    prefix_len = chunk * ring
    swap = [(i, core_count - 1 - i) for i in range(core_count)]
    q, g, k, v = queries[0], grad_out[0], keys_resp[0], values_resp[0]
    z = Shape(q, k, core_count)
    z.core_count = core_count
    if core_count == 2 and ring & (ring - 1) == 0 and ring > 1 and z.lanes * (16 * z.total + 24 * prefix_len) < 36 << 20:
        dq, red, reply = staged(z, q, g, k, v, keys_prefix, values_prefix, lengths, block_plan, ring, swap)
        return (dq[None], *red, *(x[None] for x in reply))
    qx, gx, kx, vx = (lax.ppermute(x, "resp", swap) for x in (q, g, k, v))
    mine = jnp.concatenate([keys_prefix, values_prefix], 1)
    both = lax.all_to_all(jnp.broadcast_to(mine[None], (ring,) + mine.shape), "prompt", 0, 0, tiled=True)
    both = both.reshape(prefix_len, 2 * head)
    kp, vp = both[:, :head], both[:, head:]
    core = lax.axis_index("resp").astype(jnp.int32).reshape(1)
    dq, pre, keep, send = make_kernel(core_count, z.slots, z.width, head, prefix_len)(
        block_plan[0], lengths, core, q, qx, g, gx, kp, vp, k, kx, v, vx
    )
    got = lax.ppermute(send, "resp", swap)
    parts = ring * core_count
    red = lax.all_to_all(pre.reshape(parts, prefix_len // parts, 2 * head), ("prompt", "resp"), 0, 0, tiled=True)
    red = jnp.sum(red.astype(F32), 0)
    reply = keep + got
    return (dq[None], red[:, :head], red[:, head:], reply[None, :, :head], reply[None, :, head:])


def solution(mesh):
    placed = (
        P(("groups", "prompt"), "resp", None),
        P(("groups", "prompt"), "resp", None),
        P(("groups", "prompt"), "resp", None),
        P(("groups", "prompt"), "resp", None),
        P(("groups", "prompt"), None),
        P(("groups", "prompt"), None),
        P(("groups", "prompt")),
        P(("groups", "prompt"), "resp"),
    )

    return jax.shard_map(
        local,
        mesh=mesh,
        in_specs=placed,
        out_specs=(
            P(("groups", "prompt"), "resp", None),
            P(("groups", "prompt", "resp"), None),
            P(("groups", "prompt", "resp"), None),
            P(("groups", "prompt"), "resp", None),
            P(("groups", "prompt"), "resp", None),
        ),
        check_vma=False,
    )
```
